32 devices in a mesh: dp: 16 (over z, y, core), chan: 2 (over x).
Axes of the slice: x: 2, y: 2, z: 4, core: 2. Of those that a mesh axis runs over, the one named last changes fastest.
Arguments:
- inputs: bfloat16 [768, 196, 1024], P('dp', None, 'chan'), may hold values from -6 to 6
- norm_gain: float32 [1024], P('chan'), may hold values from 0.5 to 1.5
- norm_bias: float32 [1024], P('chan'), may hold values from -3 to 3
- w_first: bfloat16 [512, 196], replicated, may hold values from -0.4375 to 0.4375
- b_first: float32 [512], replicated, may hold values from -3 to 3
- w_second: bfloat16 [196, 512], replicated, may hold values from -0.25 to 0.25
- upstream: bfloat16 [768, 196, 1024], P('dp', None, 'chan'), may hold values from -6 to 6
Outputs:
- grad_input: bfloat16 [768, 196, 1024], P('dp', None, 'chan')
- grad_first: float32 [512, 196], P('dp')
- grad_second: float32 [196, 512], P(None, 'dp')
- grad_bias_first: float32 [512], P('dp')
- grad_gain: float32 [1024], P('chan')
- grad_shift: float32 [1024], P('chan')
The draws below stay inside these ranges and needn't reach their ends.
All inputs are finite; a program needn't handle non-finite values.
Results may differ from the reference program's by a relative error of at most 0.0056.
Values sent between devices are 32-bit elements; how exact they have to be, the bound alone decides.
A program may use at most 192 MiB of HBM per device.

```python
import jax
import jax.numpy as jnp
from jax import lax

D = 1024
PATCHES = 196
TOKEN_HIDDEN = 512
B_DEV = 48
BATCH = 768
N_DP = 16


def shard_levels(key, shape, pieces, low, high):
    factor_of = 1.0
    for axis_at, shards_of in pieces:
        heights = jax.random.uniform(jax.random.fold_in(jax.random.fold_in(key, 6), axis_at), (shards_of,), jnp.float32, low / len(pieces), high / len(pieces))
        factor_of = factor_of * jnp.repeat(jnp.exp(heights), shape[axis_at] // shards_of).reshape((-1,) + (1,) * (len(shape) - 1 - axis_at))
    return factor_of


def centred(rng, shape, spread, limit, shards=(), held_as=jnp.bfloat16):
    level = shard_levels(rng, shape, shards, -0.22, 0.18) if shards else 1.0
    array = jax.random.normal(rng, shape, jnp.float32) * spread * level
    return jnp.minimum(jnp.maximum(array, -limit), limit).astype(held_as)


def setup_inputs(seed: int = 0) -> dict:
    arg_keys = jax.random.split(jax.random.key(seed), 8)
    inputs = centred(arg_keys[0], (BATCH, PATCHES, D), 1.0, 6.0, ((0, 16), (2, 2)))
    norm_gain = jnp.clip(1.0 + 0.1 * jax.random.normal(arg_keys[1], (D,), jnp.float32), 0.5, 1.5)
    norm_bias = centred(arg_keys[2], (D,), 0.5, 3.0, ((0, 2),), jnp.float32)
    w_first = centred(arg_keys[3], (TOKEN_HIDDEN, PATCHES), PATCHES ** -0.5, 0.4375)
    b_first = centred(arg_keys[4], (TOKEN_HIDDEN,), 0.5, 3.0, (), jnp.float32)
    w_second = centred(arg_keys[5], (PATCHES, TOKEN_HIDDEN), TOKEN_HIDDEN ** -0.5, 0.25)
    upstream = centred(arg_keys[6], (BATCH, PATCHES, D), 1.0, 6.0, ((0, 16), (2, 2)))
    return dict(inputs=inputs, norm_gain=norm_gain, norm_bias=norm_bias, w_first=w_first, b_first=b_first, w_second=w_second, upstream=upstream)


epsilon = 1e-06

def block_pass(values_in, upstream, norm_gain, norm_bias, w_first, b_first, w_second):
    values = values_in.astype(jnp.float32)
    row_mean = lax.optimization_barrier(jnp.mean(values, axis=-1, keepdims=True))
    centered = values - row_mean
    row_var = lax.optimization_barrier(jnp.mean(centered * centered, axis=-1, keepdims=True))
    inv_std = lax.rsqrt(row_var + epsilon)
    normed = centered * inv_std
    mixed_in = (normed * norm_gain + norm_bias).astype(jnp.bfloat16)
    pre_act = jnp.einsum('kp,bpc->bkc', w_first.astype(jnp.float32), mixed_in.astype(jnp.float32)) + b_first[None, :, None]
    gauss_cdf = 0.5 * (1.0 + lax.erf(pre_act * 0.7071067811865476))
    gauss_pdf = jnp.exp(-0.5 * pre_act * pre_act) * 0.3989422804014327
    activated = (pre_act * gauss_cdf).astype(jnp.bfloat16)
    upper = upstream.astype(jnp.float32)
    grad_act = jnp.einsum('pk,bpc->bkc', w_second.astype(jnp.float32), upper)
    grad_pre = (grad_act * (gauss_cdf + pre_act * gauss_pdf)).astype(jnp.bfloat16)
    pre_f = grad_pre.astype(jnp.float32)
    second_t = jnp.einsum('bkc,bpc->kp', activated.astype(jnp.float32), upper)
    first_w = jnp.einsum('bkc,bpc->kp', pre_f, mixed_in.astype(jnp.float32))
    first_b = lax.optimization_barrier(jnp.sum(pre_f, axis=(0, 2)))
    grad_mixed = jnp.einsum('kp,bkc->bpc', w_first.astype(jnp.float32), pre_f)
    gain_part = lax.optimization_barrier(jnp.sum(grad_mixed * normed, axis=(0, 1)))
    shift_part = lax.optimization_barrier(jnp.sum(grad_mixed, axis=(0, 1)))
    grad_normed = grad_mixed * norm_gain
    first_sum = lax.optimization_barrier(jnp.sum(grad_normed, axis=-1, keepdims=True))
    second_sum = lax.optimization_barrier(jnp.sum(grad_normed * normed, axis=-1, keepdims=True))
    grad_input = (upper + inv_std * (grad_normed - first_sum / D - normed * second_sum / D)).astype(jnp.bfloat16)
    return (grad_input, first_w, second_t, first_b, gain_part, shift_part)

def reference(inputs, norm_gain, norm_bias, w_first, b_first, w_second, upstream):
    blocks_in = inputs.reshape(N_DP, B_DEV, PATCHES, D)
    blocks_up = upstream.reshape(N_DP, B_DEV, PATCHES, D)

    def step(carry, pair):
        grad_in, first_w, second_t, first_b, gain_part, shift_part = block_pass(pair[0], pair[1], norm_gain, norm_bias, w_first, b_first, w_second)
        carry = (carry[0] + first_w, carry[1] + second_t, carry[2] + first_b, carry[3] + gain_part, carry[4] + shift_part)
        return (carry, grad_in)
    init = (jnp.zeros((TOKEN_HIDDEN, PATCHES), jnp.float32), jnp.zeros((TOKEN_HIDDEN, PATCHES), jnp.float32), jnp.zeros((TOKEN_HIDDEN,), jnp.float32), jnp.zeros((D,), jnp.float32), jnp.zeros((D,), jnp.float32))
    totals, grads = lax.scan(step, init, (blocks_in, blocks_up))
    scale = 1.0 / BATCH
    grad_input = grads.reshape(BATCH, PATCHES, D)
    return (grad_input, totals[0] * scale, (totals[1] * scale).T, totals[2] * scale, totals[3] * scale, totals[4] * scale)
```

```python
import functools

import jax
import jax.numpy as jnp
from jax import lax
from jax.experimental import pallas as pl
from jax.experimental.pallas import tpu as pltpu
from jax.sharding import PartitionSpec as P

epsilon = 1e-06
T = 16
LANES = 256
MIB = 2**20


def column(lane, p, value, held):
    return jnp.where(lane == p, value, held)


def stats_kernel(x_ref, out_ref):
    i = pl.program_id(0)
    chans = x_ref.shape[2]
    images = x_ref.shape[1]
    lane = lax.broadcasted_iota(jnp.int32, (images, out_ref.shape[2]), 1)

    @pl.when(i == 0)
    def _():
        out_ref[...] = jnp.zeros_like(out_ref)

    means, squares = out_ref[0], out_ref[1]
    for j in range(T):
        x = x_ref[j].astype(jnp.float32)
        mean = jnp.sum(x, axis=-1, keepdims=True) * (1.0 / chans)
        d = x - mean
        square = jnp.sum(d * d, axis=-1, keepdims=True)
        means = column(lane, i * T + j, mean, means)
        squares = column(lane, i * T + j, square, squares)
    out_ref[0] = means
    out_ref[1] = squares


def main_kernel(
    patches,
    x_ref,
    up_ref,
    stat_ref,
    gain_ref,
    bias_ref,
    w1_ref,
    w1t_ref,
    w2t_ref,
    gm_ref,
    sums_ref,
    gf_ref,
    gs_ref,
    chan_ref,
    mixed,
    upper,
    gmix,
):
    g = pl.program_id(0)
    images, width = stat_ref.shape[1], stat_ref.shape[2]
    chans = x_ref.shape[2]
    hidden = w1_ref.shape[0]
    padded = w1_ref.shape[1]
    full, tail = patches // T, patches % T
    f32 = jnp.float32

    @pl.when(g == 0)
    def _():
        gf_ref[...] = jnp.zeros_like(gf_ref)
        gs_ref[...] = jnp.zeros_like(gs_ref)
        chan_ref[...] = jnp.zeros_like(chan_ref)

    gain = gain_ref[...]
    bias = bias_ref[...]

    def prepare(first, count, mean, inv):
        rows = []
        for j in range(count):
            x = x_ref[first + j].astype(f32)
            normed = (x - mean[:, j : j + 1]) * inv[:, j : j + 1]
            rows.append((normed * gain + bias).astype(jnp.bfloat16))
        return rows

    def rolled(i, which):
        return pltpu.roll(stat_ref[which], lax.rem(width - i * T, width), 1)

    def step(i, _):
        first = pl.multiple_of(i * T, T)
        rows = prepare(first, T, rolled(i, 0), rolled(i, 1))
        mixed[:, pl.ds(first, T), :] = jnp.swapaxes(jnp.stack(rows), 0, 1)
        upper[:, pl.ds(first, T), :] = jnp.swapaxes(up_ref[pl.ds(first, T)], 0, 1)
        return 0

    lax.fori_loop(0, full, step, 0)
    start = full * T
    one = jnp.ones((images, chans), jnp.bfloat16)
    zero = jnp.zeros((images, chans), jnp.bfloat16)
    rows = prepare(start, tail, stat_ref[0, :, start:], stat_ref[1, :, start:]) + [one] * 3
    rows = rows + [zero] * (padded - start - len(rows))
    mixed[:, start:padded, :] = jnp.swapaxes(jnp.stack(rows), 0, 1)
    ups = [up_ref[start + j] for j in range(tail)]
    ups = ups + [zero] * (padded - start - tail)
    upper[:, start:padded, :] = jnp.swapaxes(jnp.stack(ups), 0, 1)

    block = 256
    across = (((1,), (1,)), ((), ()))

    def image(b, _):
        mb = mixed[b]
        ub = upper[b]
        total = None
        for k in range(0, hidden, block):
            ks = slice(k, k + block)
            pre = jnp.dot(w1_ref[ks, :], mb, preferred_element_type=f32)
            cdf = 0.5 * (1.0 + lax.erf(pre * 0.7071067811865476))
            pdf = jnp.exp(-0.5 * pre * pre) * 0.3989422804014327
            act = (pre * cdf).astype(jnp.bfloat16)
            ga = jnp.dot(w2t_ref[ks, :], ub, preferred_element_type=f32)
            gp = (ga * (cdf + pre * pdf)).astype(jnp.bfloat16)
            gs_ref[ks, :] += lax.dot_general(act, ub, across, preferred_element_type=f32)
            gf_ref[ks, :] += lax.dot_general(gp, mb, across, preferred_element_type=f32)
            part = jnp.dot(w1t_ref[:, ks], gp, preferred_element_type=f32)
            total = part if total is None else total + part
        gmix[b] = total
        return 0

    lax.fori_loop(0, images, image, 0)

    lane = lax.broadcasted_iota(jnp.int32, (images, width), 1)

    def finish(first, count, mean, inv, carry, tile):
        s1, s2, ga, sh = carry
        for j in range(count):
            t = tile[j]
            gm_ref[first + j] = t.astype(jnp.bfloat16)
            x = x_ref[first + j].astype(f32)
            normed = (x - mean[:, j : j + 1]) * inv[:, j : j + 1]
            tn = t * normed
            ga = ga + tn
            sh = sh + t
            s1 = column(lane, first + j, jnp.sum(t * gain, axis=-1, keepdims=True), s1)
            s2 = column(lane, first + j, jnp.sum(tn * gain, axis=-1, keepdims=True), s2)
        return s1, s2, ga, sh

    def post(i, carry):
        first = pl.multiple_of(i * T, T)
        tile = jnp.swapaxes(gmix[:, pl.ds(first, T), :], 0, 1)
        return finish(first, T, rolled(i, 0), rolled(i, 1), carry, tile)

    zs = jnp.zeros((images, width), f32)
    zc = jnp.zeros((images, chans), f32)
    carry = lax.fori_loop(0, full, post, (zs, zs, zc, zc))
    if tail:
        tile = jnp.swapaxes(gmix[:, start:padded, :], 0, 1)
        carry = finish(
            start, tail, stat_ref[0, :, start:], stat_ref[1, :, start:], carry, tile
        )
    s1, s2, ga, sh = carry
    sums_ref[0] = s1
    sums_ref[1] = s2
    chan_ref[0:1, :] += jnp.sum(ga, axis=0, keepdims=True)
    chan_ref[1:2, :] += jnp.sum(sh, axis=0, keepdims=True)


def final_kernel(x_ref, up_ref, gm_ref, stat_ref, sums_ref, gain_ref, out_ref):
    i = pl.program_id(0)
    width = stat_ref.shape[2]
    gain = gain_ref[...]
    shift = lax.rem(width - i * T, width)
    mean, inv = pltpu.roll(stat_ref[0], shift, 1), pltpu.roll(stat_ref[1], shift, 1)
    s1, s2 = pltpu.roll(sums_ref[0], shift, 1), pltpu.roll(sums_ref[1], shift, 1)
    for j in range(T):
        c = slice(j, j + 1)
        x = x_ref[j].astype(jnp.float32)
        normed = (x - mean[:, c]) * inv[:, c]
        inner = gm_ref[j].astype(jnp.float32) * gain - s1[:, c] - normed * s2[:, c]
        out_ref[j] = (up_ref[j].astype(jnp.float32) + inv[:, c] * inner).astype(jnp.bfloat16)


def others(x, axis):
    n = lax.axis_size(axis)
    return [x] + [
        lax.ppermute(x, axis, [(i, (i + s) % n) for i in range(n)]) for s in range(1, n)
    ]


def per_device(inputs, norm_gain, norm_bias, w_first, b_first, w_second, upstream):
    f32 = jnp.float32
    batch, patches, chans = inputs.shape
    hidden = w_first.shape[0]
    n_chan, n_dp = lax.axis_size("chan"), lax.axis_size("dp")
    width = chans * n_chan
    scale = 1.0 / (batch * n_dp)
    padded = -(-(patches + 3) // T) * T
    x = jnp.transpose(inputs, (1, 0, 2))
    up = jnp.transpose(upstream, (1, 0, 2))
    steps = -(-patches // T)
    S = jax.ShapeDtypeStruct
    params = functools.partial(pltpu.CompilerParams, dimension_semantics=("arbitrary",))

    local = pl.pallas_call(
        stats_kernel,
        grid=(steps,),
        in_specs=[pl.BlockSpec((T, batch, chans), lambda i: (i, 0, 0))],
        out_specs=pl.BlockSpec((2, batch, LANES), lambda i: (0, 0, 0)),
        out_shape=S((2, batch, LANES), f32),
        compiler_params=params(),
    )(x)
    every = others(local, "chan")
    mean = sum(e[0] for e in every) / n_chan
    squares = sum(e[1] for e in every) + chans * sum(
        (e[0] - mean) * (e[0] - mean) for e in every
    )
    stat = jnp.stack([mean, lax.rsqrt(squares / width + epsilon)])

    high = lax.reduce_precision(b_first, 8, 7)
    middle = lax.reduce_precision(b_first - high, 8, 7)
    low = b_first - high - middle
    extra = jnp.stack([high, middle, low], axis=1).astype(jnp.bfloat16)
    w1 = jnp.concatenate([w_first, extra], axis=1)
    w1 = jnp.pad(w1, ((0, 0), (0, padded - patches - 3)))
    w1t = jnp.pad(w_first.T, ((0, padded - patches), (0, 0)))
    w2t = jnp.pad(w_second.T, ((0, 0), (0, padded - patches)))
    gain2, bias2 = norm_gain[None, :], norm_bias[None, :]

    whole = lambda shape: pl.BlockSpec(shape, lambda g: (0,) * len(shape))
    group = T
    big = pl.BlockSpec((patches, group, chans), lambda g: (0, g, 0))
    pair = pl.BlockSpec((2, group, LANES), lambda g: (0, g, 0))
    gm, sums, gf, gs, chan = pl.pallas_call(
        functools.partial(main_kernel, patches),
        grid=(batch // group,),
        in_specs=[
            big,
            big,
            pair,
            whole((1, chans)),
            whole((1, chans)),
            whole((hidden, padded)),
            whole((padded, hidden)),
            whole((hidden, padded)),
        ],
        out_specs=[big, pair, whole((hidden, padded)), whole((hidden, padded)), whole((2, chans))],
        out_shape=[
            S((patches, batch, chans), jnp.bfloat16),
            S((2, batch, LANES), f32),
            S((hidden, padded), f32),
            S((hidden, padded), f32),
            S((2, chans), f32),
        ],
        scratch_shapes=[
            pltpu.VMEM((group, padded, chans), jnp.bfloat16),
            pltpu.VMEM((group, padded, chans), jnp.bfloat16),
            pltpu.VMEM((group, padded, chans), f32),
        ],
        compiler_params=params(vmem_limit_bytes=56 * MIB),
    )(x, up, stat, gain2, bias2, w1, w1t, w2t)

    flat = jnp.pad(chan.reshape(-1), (0, -(2 * chans) % hidden)).reshape(hidden, -1)
    packed = jnp.concatenate([gf[:, : patches + 1], gs[:, :patches], flat], axis=1)
    owned = lax.psum_scatter(packed, "dp", scatter_dimension=0, tiled=True)
    sums = sum(others(sums, "chan")) / width

    pblock = pl.BlockSpec((T, batch, chans), lambda i: (i, 0, 0))
    out = pl.pallas_call(
        final_kernel,
        grid=(steps,),
        in_specs=[
            pblock,
            pblock,
            pblock,
            whole((2, batch, LANES)),
            whole((2, batch, LANES)),
            whole((1, chans)),
        ],
        out_specs=pblock,
        out_shape=S((patches, batch, chans), jnp.bfloat16),
        compiler_params=params(),
        cost_estimate=pl.CostEstimate(
            flops=12 * x.size, bytes_accessed=8 * x.size, transcendentals=0
        ),
    )(x, up, gm, stat, sums, gain2)

    cut = 2 * patches + 1
    chan = lax.all_gather(owned[:, cut:], "dp", tiled=True)
    chan = chan.reshape(-1)[: 2 * chans].reshape(2, chans) * scale
    mine = sum(others(owned[:, :cut], "chan")) * scale
    return (
        jnp.transpose(out, (1, 0, 2)),
        mine[:, :patches],
        mine[:, patches + 1 :].T,
        mine[:, patches],
        chan[0],
        chan[1],
    )


def solution(mesh):
    in_specs = (P("dp", None, "chan"), P("chan"), P("chan"), P(), P(), P(), P("dp", None, "chan"))
    out_specs = (P("dp", None, "chan"), P("dp", None), P(None, "dp"), P("dp"), P("chan"), P("chan"))
    return jax.shard_map(
        per_device, mesh=mesh, in_specs=in_specs, out_specs=out_specs, check_vma=False
    )
```

```python
import functools

import jax
import jax.numpy as jnp
from jax import lax
from jax.experimental import pallas as pl
from jax.experimental.pallas import tpu as pltpu
from jax.sharding import PartitionSpec as P

epsilon = 1e-06
T = 16
LANES = 256
MIB = 2**20


def column(lane, p, value, held):
    return jnp.where(lane == p, value, held)


def stats_kernel(x_ref, out_ref):
    i = pl.program_id(0)
    chans = x_ref.shape[2]
    images = x_ref.shape[1]
    lane = lax.broadcasted_iota(jnp.int32, (images, out_ref.shape[2]), 1)

    @pl.when(i == 0)
    def _():
        out_ref[...] = jnp.zeros_like(out_ref)

    means, squares = out_ref[0], out_ref[1]
    rows = x_ref.shape[0]
    for j in range(rows):
        x = x_ref[j].astype(jnp.float32)
        mean = jnp.sum(x, axis=-1, keepdims=True) * (1.0 / chans)
        d = x - mean
        square = jnp.sum(d * d, axis=-1, keepdims=True)
        means = column(lane, i * rows + j, mean, means)
        squares = column(lane, i * rows + j, square, squares)
    out_ref[0] = means
    out_ref[1] = squares


def main_kernel(
    patches,
    x_ref,
    up_ref,
    stat_ref,
    gain_ref,
    bias_ref,
    w1_ref,
    w1t_ref,
    w2t_ref,
    w1f_ref,
    vec_ref,
    gm_ref,
    sums_ref,
    gf_ref,
    gs_ref,
    mixed,
    upper,
    gmix,
):
    g = pl.program_id(0)
    images, width = stat_ref.shape[1], stat_ref.shape[2]
    chans = x_ref.shape[2]
    hidden = w1_ref.shape[0]
    padded = w1_ref.shape[1]
    full, tail = patches // T, patches % T
    f32 = jnp.float32

    @pl.when(g == 0)
    def _():
        gf_ref[...] = jnp.zeros_like(gf_ref)
        gs_ref[...] = jnp.zeros_like(gs_ref)

    gain = gain_ref[...]
    bias = bias_ref[...]

    def prepare(first, count, mean, inv):
        rows = []
        for j in range(count):
            x = x_ref[first + j].astype(f32)
            normed = (x - mean[:, j : j + 1]) * inv[:, j : j + 1]
            rows.append((normed * gain + bias).astype(jnp.bfloat16))
        return rows

    def rolled(i, which):
        return pltpu.roll(stat_ref[which], lax.rem(width - i * T, width), 1)

    def step(i, _):
        first = pl.multiple_of(i * T, T)
        rows = prepare(first, T, rolled(i, 0), rolled(i, 1))
        mixed[:, pl.ds(first, T), :] = jnp.swapaxes(jnp.stack(rows), 0, 1)
        upper[:, pl.ds(first, T), :] = jnp.swapaxes(up_ref[pl.ds(first, T)], 0, 1)
        return 0

    lax.fori_loop(0, full, step, 0)
    start = full * T
    one = jnp.ones((images, chans), jnp.bfloat16)
    zero = jnp.zeros((images, chans), jnp.bfloat16)
    rows = prepare(start, tail, stat_ref[0, :, start:], stat_ref[1, :, start:]) + [one] * 3
    rows = rows + [zero] * (padded - start - len(rows))
    mixed[:, start:padded, :] = jnp.swapaxes(jnp.stack(rows), 0, 1)
    ups = [up_ref[start + j] for j in range(tail)]
    ups = ups + [zero] * (padded - start - tail)
    upper[:, start:padded, :] = jnp.swapaxes(jnp.stack(ups), 0, 1)

    block = 256
    across = (((1,), (1,)), ((), ()))

    def image(b, _):
        mb = mixed[b]
        ub = upper[b]
        total = None
        second = jnp.zeros((8, padded), f32)
        for k in range(0, hidden, block):
            ks = slice(k, k + block)
            pre = jnp.dot(w1_ref[ks, :], mb, preferred_element_type=f32)
            ga = jnp.dot(w2t_ref[ks, :], ub, preferred_element_type=f32)
            u = pre * 0.7071067811865476
            twice = 1.0 + lax.erf(u)
            slope = (u * 1.1283791670955126) * jnp.exp2(u * u * -1.4426950408889634)
            act = (pre * twice).astype(jnp.bfloat16)
            gp = (ga * (twice + slope)).astype(jnp.bfloat16)
            gs_ref[ks, :] += lax.dot_general(act, ub, across, preferred_element_type=f32)
            gf = lax.dot_general(gp, mb, across, preferred_element_type=f32)
            gf_ref[ks, :] += gf
            second = second + jnp.sum((gf * w1f_ref[ks, :]).reshape(-1, 8, padded), axis=0)
            part = jnp.dot(w1t_ref[:, ks], gp, preferred_element_type=f32)
            total = part if total is None else total + part
        rounded = total.astype(jnp.bfloat16)
        gmix[b] = rounded
        dots = lax.dot_general(vec_ref[...], rounded, across, preferred_element_type=f32)
        second = jnp.sum(second, axis=0, keepdims=True)
        sums_ref[0, pl.ds(b, 1), :padded] = dots[0:1] + dots[1:2]
        sums_ref[1, pl.ds(b, 1), :padded] = second - (dots[2:3] + dots[3:4])
        return 0

    lax.fori_loop(0, images, image, 0)

    def post(i, _):
        first = pl.multiple_of(i * T, T)
        gm_ref[pl.ds(first, T)] = jnp.swapaxes(gmix[:, pl.ds(first, T), :], 0, 1)
        return 0

    lax.fori_loop(0, full, post, 0)
    if tail:
        tile = jnp.swapaxes(gmix[:, start:padded, :], 0, 1)
        gm_ref[start:] = tile[:tail]


def final_kernel(x_ref, up_ref, gm_ref, stat_ref, sums_ref, gain_ref, out_ref, chan_ref):
    i = pl.program_id(0)
    rows = x_ref.shape[0]
    width = stat_ref.shape[2]
    gain = gain_ref[...]

    @pl.when(i == 0)
    def _():
        chan_ref[...] = jnp.zeros_like(chan_ref)

    shift = lax.rem(width - i * rows, width)
    mean, inv = pltpu.roll(stat_ref[0], shift, 1), pltpu.roll(stat_ref[1], shift, 1)
    s1, s2 = pltpu.roll(sums_ref[0], shift, 1), pltpu.roll(sums_ref[1], shift, 1)
    products = jnp.zeros(x_ref.shape[1:], jnp.float32)
    plain = jnp.zeros(x_ref.shape[1:], jnp.float32)
    for j in range(rows):
        c = slice(j, j + 1)
        x = x_ref[j].astype(jnp.float32)
        normed = (x - mean[:, c]) * inv[:, c]
        t = gm_ref[j].astype(jnp.float32)
        products = products + t * normed
        plain = plain + t
        inner = t * gain - s1[:, c] - normed * s2[:, c]
        out_ref[j] = (up_ref[j].astype(jnp.float32) + inv[:, c] * inner).astype(jnp.bfloat16)
    chan_ref[0:1, :] += jnp.sum(products, axis=0, keepdims=True)
    chan_ref[1:2, :] += jnp.sum(plain, axis=0, keepdims=True)


def reduce_kernel(scale, first_ref, second_ref, chan_ref, out_ref, chan_out_ref, *scratch):
    one, one_c, held, held_c, two, two_c, own, three, sems, sems2, sems3 = scratch
    me, col = lax.axis_index("dp"), lax.axis_index("chan")
    n_dp, n_chan = lax.axis_size("dp"), lax.axis_size("chan")
    halves = n_dp // 2
    mine, core = me // 2, me % 2
    partner = me + 1 - 2 * core
    peers = [((mine + j) % halves) * 2 + core for j in range(1, halves)]
    columns = [(col + s) % n_chan for s in range(1, n_chan)]
    mesh_id = pl.DeviceIdType.MESH

    barrier = pltpu.get_barrier_semaphore()
    for d in [partner] + peers:
        pl.semaphore_signal(barrier, inc=1, device_id=(d, col), device_id_type=mesh_id)
    for d in columns:
        pl.semaphore_signal(barrier, inc=1, device_id=(me, d), device_id_type=mesh_id)
    pl.semaphore_wait(barrier, halves + n_chan - 1)

    def send(src, dst, sem, k, target):
        copy = pltpu.make_async_remote_copy(
            src_ref=src,
            dst_ref=dst,
            send_sem=sem.at[0, k],
            recv_sem=sem.at[1, k],
            device_id=target,
            device_id_type=mesh_id,
        )
        copy.start()
        return copy

    copies = [
        send(first_ref.at[:, 1 - core], one.at[0], sems, 0, (partner, col)),
        send(second_ref.at[:, 1 - core], one.at[1], sems, 1, (partner, col)),
        send(chan_ref, one_c, sems, 2, (partner, col)),
    ]
    for c in copies:
        c.wait()

    def add(t, _):
        held[t, 0] = first_ref[t, core] + one[0, t]
        held[t, 1] = second_ref[t, core] + one[1, t]
        return 0

    lax.fori_loop(0, halves, add, 0)
    held_c[...] = chan_ref[...] + one_c[...]
    copies = []
    for j in range(1, halves):
        t = (mine + j) % halves
        copies.append(send(held.at[t], two.at[j - 1], sems2, 2 * j - 2, (2 * t + core, col)))
        copies.append(send(held_c, two_c.at[mine], sems2, 2 * j - 1, (2 * t + core, col)))
    two_c[mine] = held_c[...]
    for c in copies:
        c.wait()
    total = held[mine]
    for j in range(1, halves):
        total = total + two[j - 1]
    own[...] = total
    copies = [
        send(own, three.at[col], sems3, s, (me, d)) for s, d in enumerate(columns)
    ]
    three[col] = total
    chan_sum = two_c[0]
    for j in range(1, halves):
        chan_sum = chan_sum + two_c[j]
    chan_out_ref[...] = chan_sum * scale
    for c in copies:
        c.wait()
    total = three[0]
    for j in range(1, n_chan):
        total = total + three[j]
    out_ref[...] = total * scale


def reduce_all(first, second, chan, scale):
    n_dp, n_chan = lax.axis_size("dp"), lax.axis_size("chan")
    halves = n_dp // 2
    rows, lanes = first.shape[0] // n_dp, first.shape[1]
    f32 = jnp.float32
    S = jax.ShapeDtypeStruct
    vmem = pl.BlockSpec(memory_space=pltpu.VMEM)
    shape = (halves, 2, rows, lanes)
    dma = pltpu.SemaphoreType.DMA
    return pl.pallas_call(
        functools.partial(reduce_kernel, scale),
        in_specs=[vmem] * 3,
        out_specs=[vmem] * 2,
        out_shape=[S((2, rows, lanes), f32), S(chan.shape, f32)],
        scratch_shapes=[
            pltpu.VMEM((2, halves, rows, lanes), f32),
            pltpu.VMEM(chan.shape, f32),
            pltpu.VMEM(shape, f32),
            pltpu.VMEM(chan.shape, f32),
            pltpu.VMEM((halves - 1, 2, rows, lanes), f32),
            pltpu.VMEM((halves,) + chan.shape, f32),
            pltpu.VMEM((2, rows, lanes), f32),
            pltpu.VMEM((n_chan, 2, rows, lanes), f32),
            dma((2, 3)),
            dma((2, 2 * halves - 2)),
            dma((2, n_chan - 1)),
        ],
        compiler_params=pltpu.CompilerParams(collective_id=0, has_side_effects=True),
    )(first.reshape(shape), second.reshape(shape), chan)


def others(x, axis):
    n = lax.axis_size(axis)
    return [x] + [
        lax.ppermute(x, axis, [(i, (i + s) % n) for i in range(n)]) for s in range(1, n)
    ]


def per_device(inputs, norm_gain, norm_bias, w_first, b_first, w_second, upstream):
    f32 = jnp.float32
    batch, patches, chans = inputs.shape
    hidden = w_first.shape[0]
    n_chan, n_dp = lax.axis_size("chan"), lax.axis_size("dp")
    width = chans * n_chan
    scale = 1.0 / (batch * n_dp)
    padded = -(-(patches + 3) // T) * T
    x = jnp.transpose(inputs, (1, 0, 2))
    up = jnp.transpose(upstream, (1, 0, 2))
    rows = max(r for r in range(1, T + 1) if patches % r == 0)
    steps = patches // rows
    S = jax.ShapeDtypeStruct
    params = functools.partial(pltpu.CompilerParams, dimension_semantics=("arbitrary",))

    local = pl.pallas_call(
        stats_kernel,
        grid=(steps,),
        in_specs=[pl.BlockSpec((rows, batch, chans), lambda i: (i, 0, 0))],
        out_specs=pl.BlockSpec((2, batch, LANES), lambda i: (0, 0, 0)),
        out_shape=S((2, batch, LANES), f32),
        compiler_params=params(),
    )(x)
    every = others(local, "chan")
    mean = sum(e[0] for e in every) / n_chan
    squares = sum(e[1] for e in every) + chans * sum(
        (e[0] - mean) * (e[0] - mean) for e in every
    )
    stat = jnp.stack([mean, lax.rsqrt(squares / width + epsilon)])

    high = lax.reduce_precision(b_first, 8, 7)
    middle = lax.reduce_precision(b_first - high, 8, 7)
    low = b_first - high - middle
    extra = jnp.stack([high, middle, low], axis=1).astype(jnp.bfloat16)
    w1 = jnp.concatenate([w_first, extra], axis=1)
    w1 = jnp.pad(w1, ((0, 0), (0, padded - patches - 3)))
    w1t = jnp.pad(w_first.T, ((0, padded - patches), (0, 0)))
    w2t = jnp.pad(0.5 * w_second.T, ((0, 0), (0, padded - patches)))
    w1f = w1t.T.astype(f32)
    gain2, bias2 = norm_gain[None, :], norm_bias[None, :]
    lead = lax.reduce_precision(jnp.stack([norm_gain, norm_bias]), 8, 7)
    rest = jnp.stack([norm_gain, norm_bias]) - lead
    vec = jnp.stack([lead[0], rest[0], lead[1], rest[1]]).astype(jnp.bfloat16)
    vec = jnp.pad(vec, ((0, T - 4), (0, 0)))

    whole = lambda shape: pl.BlockSpec(shape, lambda g: (0,) * len(shape))
    group = T
    big = pl.BlockSpec((patches, group, chans), lambda g: (0, g, 0))
    pair = pl.BlockSpec((2, group, LANES), lambda g: (0, g, 0))
    gm, sums, gf, gs = pl.pallas_call(
        functools.partial(main_kernel, patches),
        grid=(batch // group,),
        in_specs=[
            big,
            big,
            pair,
            whole((1, chans)),
            whole((1, chans)),
            whole((hidden, padded)),
            whole((padded, hidden)),
            whole((hidden, padded)),
            whole((hidden, padded)),
            whole((T, chans)),
        ],
        out_specs=[big, pair, whole((hidden, padded)), whole((hidden, padded))],
        out_shape=[
            S((patches, batch, chans), jnp.bfloat16),
            S((2, batch, LANES), f32),
            S((hidden, padded), f32),
            S((hidden, padded), f32),
        ],
        scratch_shapes=[
            pltpu.VMEM((group, padded, chans), jnp.bfloat16),
            pltpu.VMEM((group, padded, chans), jnp.bfloat16),
            pltpu.VMEM((group, padded, chans), jnp.bfloat16),
        ],
        compiler_params=params(vmem_limit_bytes=56 * MIB),
    )(x, up, stat, gain2, bias2, w1, w1t, w2t, w1f, vec)

    sums = sum(others(sums, "chan")) / width

    pblock = pl.BlockSpec((rows, batch, chans), lambda i: (i, 0, 0))
    out, chan = pl.pallas_call(
        final_kernel,
        grid=(steps,),
        in_specs=[
            pblock,
            pblock,
            pblock,
            whole((2, batch, LANES)),
            whole((2, batch, LANES)),
            whole((1, chans)),
        ],
        out_specs=[pblock, whole((2, chans))],
        out_shape=[S((patches, batch, chans), jnp.bfloat16), S((2, chans), f32)],
        compiler_params=params(),
        cost_estimate=pl.CostEstimate(
            flops=12 * x.size, bytes_accessed=8 * x.size, transcendentals=0
        ),
    )(x, up, gm, stat, sums, gain2)

    mine, chan = reduce_all(gf, gs, chan, scale)
    return (
        jnp.transpose(out, (1, 0, 2)),
        mine[0, :, :patches],
        (0.5 * mine[1, :, :patches]).T,
        mine[0, :, patches],
        chan[0],
        chan[1],
    )


def solution(mesh):
    in_specs = (P("dp", None, "chan"), P("chan"), P("chan"), P(), P(), P(), P("dp", None, "chan"))
    out_specs = (P("dp", None, "chan"), P("dp", None), P(None, "dp"), P("dp"), P("chan"), P("chan"))
    return jax.shard_map(
        per_device, mesh=mesh, in_specs=in_specs, out_specs=out_specs, check_vma=False
    )
```

```python
import functools

import jax
import jax.numpy as jnp
from jax import lax
from jax.experimental import pallas as pl
from jax.experimental.pallas import tpu as pltpu
from jax.sharding import PartitionSpec as P

epsilon = 1e-06
T = 16
LANES = 256
SIDE = 128
MIB = 2**20


def column(lane, p, value, held):
    return jnp.where(lane == p, value, held)


def stats_kernel(x_ref, out_ref):
    i = pl.program_id(0)
    chans = x_ref.shape[2]
    images = x_ref.shape[1]
    lane = lax.broadcasted_iota(jnp.int32, (images, out_ref.shape[2]), 1)

    @pl.when(i == 0)
    def _():
        out_ref[...] = jnp.zeros_like(out_ref)

    f32 = jnp.float32
    rows = x_ref.shape[0]
    x = x_ref[...].reshape(rows * images, chans)
    mean = jnp.dot(x, jnp.ones((chans, SIDE), jnp.bfloat16), preferred_element_type=f32)
    mean = mean * (1.0 / chans)
    square = jnp.zeros_like(mean)
    for k in range(0, chans, SIDE):
        d = x[:, k : k + SIDE].astype(f32) - mean
        square = square + d * d
    high = square.astype(jnp.bfloat16)
    low = (square - high.astype(f32)).astype(jnp.bfloat16)
    ones = jnp.ones((SIDE, SIDE), jnp.bfloat16)
    square = jnp.dot(high, ones, preferred_element_type=f32) + jnp.dot(
        low, ones, preferred_element_type=f32
    )
    means, squares = out_ref[0], out_ref[1]
    for j in range(rows):
        part = slice(j * images, (j + 1) * images)
        m = jnp.concatenate([mean[part]] * (LANES // SIDE), axis=1)
        q = jnp.concatenate([square[part]] * (LANES // SIDE), axis=1)
        means = column(lane, i * rows + j, m, means)
        squares = column(lane, i * rows + j, q, squares)
    out_ref[0] = means
    out_ref[1] = squares


def spread(value, count, chans):
    f32 = jnp.float32
    n = value.shape[0]
    v = value[:, :SIDE]
    lane = lax.broadcasted_iota(jnp.int32, v.shape, 1)
    high = v.astype(jnp.bfloat16).astype(f32)
    middle = (v - high).astype(jnp.bfloat16).astype(f32)
    low = v - high - middle
    placed = jnp.where(lane < 64, pltpu.roll(middle, 32, 1), pltpu.roll(low, 64, 1))
    placed = jnp.where(lane < 32, high, placed)
    lane = jnp.where(lane < 96, lax.rem(lane, 32), 32)
    picks = [jnp.where(lane == j, placed, 0.0).astype(jnp.bfloat16) for j in range(count)]
    ones = jnp.ones((SIDE, SIDE), jnp.bfloat16)
    out = jnp.dot(jnp.concatenate(picks, axis=0), ones, preferred_element_type=f32)
    return [
        jnp.concatenate([out[j * n : (j + 1) * n]] * (chans // SIDE), axis=1)
        for j in range(count)
    ]


def main_kernel(
    patches,
    x_ref,
    up_ref,
    stat_ref,
    gain_ref,
    bias_ref,
    w1_ref,
    w1t_ref,
    w2t_ref,
    w1f_ref,
    vec_ref,
    gm_ref,
    sums_ref,
    gf_ref,
    gs_ref,
    mixed,
    upper,
    gmix,
):
    g = pl.program_id(0)
    images, width = stat_ref.shape[1], stat_ref.shape[2]
    chans = x_ref.shape[2]
    hidden = w1_ref.shape[0]
    padded = w1_ref.shape[1]
    full, tail = patches // T, patches % T
    f32 = jnp.float32

    @pl.when(g == 0)
    def _():
        gf_ref[...] = jnp.zeros_like(gf_ref)
        gs_ref[...] = jnp.zeros_like(gs_ref)

    gain = gain_ref[...]
    bias = bias_ref[...]

    def prepare(first, count, mean, inv):
        rows = []
        mean, inv = spread(mean, count, chans), spread(inv, count, chans)
        for j in range(count):
            x = x_ref[first + j].astype(f32)
            normed = (x - mean[j]) * inv[j]
            rows.append((normed * gain + bias).astype(jnp.bfloat16))
        return rows

    def rolled(i, which):
        return pltpu.roll(stat_ref[which], lax.rem(width - i * T, width), 1)

    def step(i, _):
        first = pl.multiple_of(i * T, T)
        rows = prepare(first, T, rolled(i, 0), rolled(i, 1))
        mixed[:, pl.ds(first, T), :] = jnp.swapaxes(jnp.stack(rows), 0, 1)
        upper[:, pl.ds(first, T), :] = jnp.swapaxes(up_ref[pl.ds(first, T)], 0, 1)
        return 0

    lax.fori_loop(0, full, step, 0)
    start = full * T
    one = jnp.ones((images, chans), jnp.bfloat16)
    zero = jnp.zeros((images, chans), jnp.bfloat16)
    rows = prepare(start, tail, rolled(full, 0), rolled(full, 1)) if tail else []
    rows = rows + [one] * 3
    rows = rows + [zero] * (padded - start - len(rows))
    mixed[:, start:padded, :] = jnp.swapaxes(jnp.stack(rows), 0, 1)
    ups = [up_ref[start + j] for j in range(tail)]
    ups = ups + [zero] * (padded - start - tail)
    upper[:, start:padded, :] = jnp.swapaxes(jnp.stack(ups), 0, 1)

    block = 256
    across = (((1,), (1,)), ((), ()))

    def image(b, _):
        mb = mixed[b]
        ub = upper[b]
        total = None
        second = jnp.zeros((8, padded), f32)
        for k in range(0, hidden, block):
            ks = slice(k, k + block)
            pre = jnp.dot(w1_ref[ks, :], mb, preferred_element_type=f32)
            ga = jnp.dot(w2t_ref[ks, :], ub, preferred_element_type=f32)
            u = pre * 0.7071067811865476
            twice = 1.0 + lax.erf(u)
            slope = (u * 1.1283791670955126) * jnp.exp2(u * u * -1.4426950408889634)
            act = (pre * twice).astype(jnp.bfloat16)
            gp = (ga * (twice + slope)).astype(jnp.bfloat16)
            gs_ref[ks, :] += lax.dot_general(act, ub, across, preferred_element_type=f32)
            gf = lax.dot_general(gp, mb, across, preferred_element_type=f32)
            gf_ref[ks, :] += gf
            second = second + jnp.sum((gf * w1f_ref[ks, :]).reshape(-1, 8, padded), axis=0)
            part = jnp.dot(w1t_ref[:, ks], gp, preferred_element_type=f32)
            total = part if total is None else total + part
        rounded = total.astype(jnp.bfloat16)
        gmix[b] = rounded
        dots = lax.dot_general(vec_ref[...], rounded, across, preferred_element_type=f32)
        second = jnp.sum(second, axis=0, keepdims=True)
        sums_ref[0, pl.ds(b, 1), :padded] = dots[0:1] + dots[1:2]
        sums_ref[1, pl.ds(b, 1), :padded] = second - (dots[2:3] + dots[3:4])
        return 0

    lax.fori_loop(0, images, image, 0)

    def post(i, _):
        first = pl.multiple_of(i * T, T)
        gm_ref[pl.ds(first, T)] = jnp.swapaxes(gmix[:, pl.ds(first, T), :], 0, 1)
        return 0

    lax.fori_loop(0, full, post, 0)
    if tail:
        tile = jnp.swapaxes(gmix[:, start:padded, :], 0, 1)
        gm_ref[start:] = tile[:tail]


def final_kernel(x_ref, up_ref, gm_ref, stat_ref, sums_ref, gain_ref, out_ref, chan_ref):
    i = pl.program_id(0)
    rows = x_ref.shape[0]
    width = stat_ref.shape[2]
    gain = gain_ref[...]

    @pl.when(i == 0)
    def _():
        chan_ref[...] = jnp.zeros_like(chan_ref)

    shift = lax.rem(width - i * rows, width)
    chans = x_ref.shape[2]
    raw = pltpu.roll(stat_ref[1], shift, 1)
    mean = spread(pltpu.roll(stat_ref[0], shift, 1), rows, chans)
    inv = spread(raw, rows, chans)
    s1 = spread(raw * pltpu.roll(sums_ref[0], shift, 1), rows, chans)
    s2 = spread(raw * pltpu.roll(sums_ref[1], shift, 1), rows, chans)
    products = jnp.zeros(x_ref.shape[1:], jnp.float32)
    plain = jnp.zeros(x_ref.shape[1:], jnp.float32)
    for j in range(rows):
        x = x_ref[j].astype(jnp.float32)
        normed = (x - mean[j]) * inv[j]
        t = gm_ref[j].astype(jnp.float32)
        products = products + t * normed
        plain = plain + t
        inner = t * gain * inv[j] - s1[j] - normed * s2[j]
        out_ref[j] = (up_ref[j].astype(jnp.float32) + inner).astype(jnp.bfloat16)
    chan_ref[0:1, :] += jnp.sum(products, axis=0, keepdims=True)
    chan_ref[1:2, :] += jnp.sum(plain, axis=0, keepdims=True)


def reduce_kernel(scale, first_ref, second_ref, chan_ref, out_ref, chan_out_ref, *scratch):
    one, one_c, held, held_c, two, two_c, own, three, sems, sems2, sems3 = scratch
    me, col = lax.axis_index("dp"), lax.axis_index("chan")
    n_dp, n_chan = lax.axis_size("dp"), lax.axis_size("chan")
    halves = n_dp // 2
    mine, core = me // 2, me % 2
    partner = me + 1 - 2 * core
    peers = [((mine + j) % halves) * 2 + core for j in range(1, halves)]
    columns = [(col + s) % n_chan for s in range(1, n_chan)]
    mesh_id = pl.DeviceIdType.MESH

    barrier = pltpu.get_barrier_semaphore()
    for d in [partner] + peers:
        pl.semaphore_signal(barrier, inc=1, device_id=(d, col), device_id_type=mesh_id)
    for d in columns:
        pl.semaphore_signal(barrier, inc=1, device_id=(me, d), device_id_type=mesh_id)
    pl.semaphore_wait(barrier, halves + n_chan - 1)

    def send(src, dst, sem, k, target):
        copy = pltpu.make_async_remote_copy(
            src_ref=src,
            dst_ref=dst,
            send_sem=sem.at[0, k],
            recv_sem=sem.at[1, k],
            device_id=target,
            device_id_type=mesh_id,
        )
        copy.start()
        return copy

    copies = [
        send(first_ref.at[:, 1 - core], one.at[0], sems, 0, (partner, col)),
        send(second_ref.at[:, 1 - core], one.at[1], sems, 1, (partner, col)),
        send(chan_ref, one_c, sems, 2, (partner, col)),
    ]
    for c in copies:
        c.wait()

    def add(t, _):
        held[t, 0] = first_ref[t, core] + one[0, t]
        held[t, 1] = second_ref[t, core] + one[1, t]
        return 0

    lax.fori_loop(0, halves, add, 0)
    held_c[...] = chan_ref[...] + one_c[...]
    copies = []
    for j in range(1, halves):
        t = (mine + j) % halves
        copies.append(send(held.at[t], two.at[j - 1], sems2, 2 * j - 2, (2 * t + core, col)))
        copies.append(send(held_c, two_c.at[mine], sems2, 2 * j - 1, (2 * t + core, col)))
    two_c[mine] = held_c[...]
    for c in copies:
        c.wait()
    total = held[mine]
    for j in range(1, halves):
        total = total + two[j - 1]
    own[...] = total
    copies = [
        send(own, three.at[col], sems3, s, (me, d)) for s, d in enumerate(columns)
    ]
    three[col] = total
    chan_sum = two_c[0]
    for j in range(1, halves):
        chan_sum = chan_sum + two_c[j]
    chan_out_ref[...] = chan_sum * scale
    for c in copies:
        c.wait()
    total = three[0]
    for j in range(1, n_chan):
        total = total + three[j]
    out_ref[...] = total * scale


def reduce_all(first, second, chan, scale):
    n_dp, n_chan = lax.axis_size("dp"), lax.axis_size("chan")
    halves = n_dp // 2
    rows, lanes = first.shape[0] // n_dp, first.shape[1]
    f32 = jnp.float32
    S = jax.ShapeDtypeStruct
    vmem = pl.BlockSpec(memory_space=pltpu.VMEM)
    shape = (halves, 2, rows, lanes)
    dma = pltpu.SemaphoreType.DMA
    return pl.pallas_call(
        functools.partial(reduce_kernel, scale),
        in_specs=[vmem] * 3,
        out_specs=[vmem] * 2,
        out_shape=[S((2, rows, lanes), f32), S(chan.shape, f32)],
        scratch_shapes=[
            pltpu.VMEM((2, halves, rows, lanes), f32),
            pltpu.VMEM(chan.shape, f32),
            pltpu.VMEM(shape, f32),
            pltpu.VMEM(chan.shape, f32),
            pltpu.VMEM((halves - 1, 2, rows, lanes), f32),
            pltpu.VMEM((halves,) + chan.shape, f32),
            pltpu.VMEM((2, rows, lanes), f32),
            pltpu.VMEM((n_chan, 2, rows, lanes), f32),
            dma((2, 3)),
            dma((2, 2 * halves - 2)),
            dma((2, n_chan - 1)),
        ],
        compiler_params=pltpu.CompilerParams(collective_id=0, has_side_effects=True),
    )(first.reshape(shape), second.reshape(shape), chan)


def others(x, axis):
    n = lax.axis_size(axis)
    return [x] + [
        lax.ppermute(x, axis, [(i, (i + s) % n) for i in range(n)]) for s in range(1, n)
    ]


def per_device(inputs, norm_gain, norm_bias, w_first, b_first, w_second, upstream):
    f32 = jnp.float32
    batch, patches, chans = inputs.shape
    hidden = w_first.shape[0]
    n_chan, n_dp = lax.axis_size("chan"), lax.axis_size("dp")
    width = chans * n_chan
    scale = 1.0 / (batch * n_dp)
    padded = -(-(patches + 3) // T) * T
    x = jnp.transpose(inputs, (1, 0, 2))
    up = jnp.transpose(upstream, (1, 0, 2))
    rows = max(r for r in range(1, T + 1) if patches % r == 0)
    steps = patches // rows
    S = jax.ShapeDtypeStruct
    params = functools.partial(pltpu.CompilerParams, dimension_semantics=("arbitrary",))

    local = pl.pallas_call(
        stats_kernel,
        grid=(steps,),
        in_specs=[pl.BlockSpec((rows, batch, chans), lambda i: (i, 0, 0))],
        out_specs=pl.BlockSpec((2, batch, LANES), lambda i: (0, 0, 0)),
        out_shape=S((2, batch, LANES), f32),
        compiler_params=params(),
    )(x)
    every = others(local, "chan")
    mean = sum(e[0] for e in every) / n_chan
    squares = sum(e[1] for e in every) + chans * sum(
        (e[0] - mean) * (e[0] - mean) for e in every
    )
    stat = jnp.stack([mean, lax.rsqrt(squares / width + epsilon)])

    high = lax.reduce_precision(b_first, 8, 7)
    middle = lax.reduce_precision(b_first - high, 8, 7)
    low = b_first - high - middle
    extra = jnp.stack([high, middle, low], axis=1).astype(jnp.bfloat16)
    w1 = jnp.concatenate([w_first, extra], axis=1)
    w1 = jnp.pad(w1, ((0, 0), (0, padded - patches - 3)))
    w1t = jnp.pad(w_first.T, ((0, padded - patches), (0, 0)))
    w2t = jnp.pad(0.5 * w_second.T, ((0, 0), (0, padded - patches)))
    w1f = w1t.T.astype(f32)
    gain2, bias2 = norm_gain[None, :], norm_bias[None, :]
    lead = lax.reduce_precision(jnp.stack([norm_gain, norm_bias]), 8, 7)
    rest = jnp.stack([norm_gain, norm_bias]) - lead
    vec = jnp.stack([lead[0], rest[0], lead[1], rest[1]]).astype(jnp.bfloat16)
    vec = jnp.pad(vec, ((0, T - 4), (0, 0)))

    whole = lambda shape: pl.BlockSpec(shape, lambda g: (0,) * len(shape))
    group = T
    big = pl.BlockSpec((patches, group, chans), lambda g: (0, g, 0))
    pair = pl.BlockSpec((2, group, LANES), lambda g: (0, g, 0))
    gm, sums, gf, gs = pl.pallas_call(
        functools.partial(main_kernel, patches),
        grid=(batch // group,),
        in_specs=[
            big,
            big,
            pair,
            whole((1, chans)),
            whole((1, chans)),
            whole((hidden, padded)),
            whole((padded, hidden)),
            whole((hidden, padded)),
            whole((hidden, padded)),
            whole((T, chans)),
        ],
        out_specs=[big, pair, whole((hidden, padded)), whole((hidden, padded))],
        out_shape=[
            S((patches, batch, chans), jnp.bfloat16),
            S((2, batch, LANES), f32),
            S((hidden, padded), f32),
            S((hidden, padded), f32),
        ],
        scratch_shapes=[
            pltpu.VMEM((group, padded, chans), jnp.bfloat16),
            pltpu.VMEM((group, padded, chans), jnp.bfloat16),
            pltpu.VMEM((group, padded, chans), jnp.bfloat16),
        ],
        compiler_params=params(vmem_limit_bytes=56 * MIB),
    )(x, up, stat, gain2, bias2, w1, w1t, w2t, w1f, vec)

    sums = sum(others(sums, "chan")) / width

    pblock = pl.BlockSpec((rows, batch, chans), lambda i: (i, 0, 0))
    out, chan = pl.pallas_call(
        final_kernel,
        grid=(steps,),
        in_specs=[
            pblock,
            pblock,
            pblock,
            whole((2, batch, LANES)),
            whole((2, batch, LANES)),
            whole((1, chans)),
        ],
        out_specs=[pblock, whole((2, chans))],
        out_shape=[S((patches, batch, chans), jnp.bfloat16), S((2, chans), f32)],
        compiler_params=params(),
        cost_estimate=pl.CostEstimate(
            flops=12 * x.size, bytes_accessed=8 * x.size, transcendentals=0
        ),
    )(x, up, gm, stat, sums, gain2)

    mine, chan = reduce_all(gf, gs, chan, scale)
    return (
        jnp.transpose(out, (1, 0, 2)),
        mine[0, :, :patches],
        (0.5 * mine[1, :, :patches]).T,
        mine[0, :, patches],
        chan[0],
        chan[1],
    )


def solution(mesh):
    in_specs = (P("dp", None, "chan"), P("chan"), P("chan"), P(), P(), P(), P("dp", None, "chan"))
    out_specs = (P("dp", None, "chan"), P("dp", None), P(None, "dp"), P("dp"), P("chan"), P("chan"))
    return jax.shard_map(
        per_device, mesh=mesh, in_specs=in_specs, out_specs=out_specs, check_vma=False
    )
```

```python
import functools

import jax
import jax.numpy as jnp
from jax import lax
from jax.experimental import pallas as pl
from jax.experimental.pallas import tpu as pltpu
from jax.sharding import PartitionSpec as P

epsilon = 1e-06
T = 16
LANES = 256
MIB = 2**20


def column(lane, p, value, held):
    return jnp.where(lane == p, value, held)


def stats_kernel(x_ref, out_ref):
    i = pl.program_id(0)
    chans = x_ref.shape[2]
    images = x_ref.shape[1]
    lane = lax.broadcasted_iota(jnp.int32, (images, out_ref.shape[2]), 1)

    @pl.when(i == 0)
    def _():
        out_ref[...] = jnp.zeros_like(out_ref)

    means, squares = out_ref[0], out_ref[1]
    rows = x_ref.shape[0]
    for j in range(rows):
        x = x_ref[j].astype(jnp.float32)
        mean = jnp.sum(x, axis=-1, keepdims=True) * (1.0 / chans)
        d = x - mean
        square = jnp.sum(d * d, axis=-1, keepdims=True)
        means = column(lane, i * rows + j, mean, means)
        squares = column(lane, i * rows + j, square, squares)
    out_ref[0] = means
    out_ref[1] = squares


def main_kernel(
    patches,
    x_ref,
    up_ref,
    stat_ref,
    gain_ref,
    bias_ref,
    w1_ref,
    w1t_ref,
    w2t_ref,
    w1f_ref,
    vec_ref,
    gm_ref,
    sums_ref,
    gf_ref,
    gs_ref,
    mixed,
    upper,
    gmix,
):
    g = pl.program_id(0)
    images, width = stat_ref.shape[1], stat_ref.shape[2]
    chans = x_ref.shape[2]
    hidden = w1_ref.shape[0]
    padded = w1_ref.shape[1]
    full, tail = patches // T, patches % T
    f32 = jnp.float32

    @pl.when(g == 0)
    def _():
        gf_ref[...] = jnp.zeros_like(gf_ref)
        gs_ref[...] = jnp.zeros_like(gs_ref)

    gain = gain_ref[...]
    bias = bias_ref[...]

    def prepare(first, count, mean, inv):
        rows = []
        for j in range(count):
            x = x_ref[first + j].astype(f32)
            normed = (x - mean[:, j : j + 1]) * inv[:, j : j + 1]
            rows.append((normed * gain + bias).astype(jnp.bfloat16))
        return rows

    def rolled(i, which):
        return pltpu.roll(stat_ref[which], lax.rem(width - i * T, width), 1)

    def step(i, _):
        first = pl.multiple_of(i * T, T)
        rows = prepare(first, T, rolled(i, 0), rolled(i, 1))
        mixed[:, pl.ds(first, T), :] = jnp.swapaxes(jnp.stack(rows), 0, 1)
        upper[:, pl.ds(first, T), :] = jnp.swapaxes(up_ref[pl.ds(first, T)], 0, 1)
        return 0

    lax.fori_loop(0, full, step, 0)
    start = full * T
    one = jnp.ones((images, chans), jnp.bfloat16)
    zero = jnp.zeros((images, chans), jnp.bfloat16)
    rows = prepare(start, tail, stat_ref[0, :, start:], stat_ref[1, :, start:]) + [one] * 3
    rows = rows + [zero] * (padded - start - len(rows))
    mixed[:, start:padded, :] = jnp.swapaxes(jnp.stack(rows), 0, 1)
    ups = [up_ref[start + j] for j in range(tail)]
    ups = ups + [zero] * (padded - start - tail)
    upper[:, start:padded, :] = jnp.swapaxes(jnp.stack(ups), 0, 1)

    block = hidden
    across = (((1,), (1,)), ((), ()))

    def image(b, _):
        mb = mixed[b]
        ub = upper[b]
        total = None
        second = jnp.zeros((8, padded), f32)
        for k in range(0, hidden, block):
            ks = slice(k, k + block)
            pre = jnp.dot(w1_ref[ks, :], mb, preferred_element_type=f32)
            ga = jnp.dot(w2t_ref[ks, :], ub, preferred_element_type=f32)
            u = pre * 0.7071067811865476
            twice = 1.0 + lax.erf(u)
            slope = (u * 1.1283791670955126) * jnp.exp2(u * u * -1.4426950408889634)
            act = (pre * twice).astype(jnp.bfloat16)
            gp = (ga * (twice + slope)).astype(jnp.bfloat16)
            gs_ref[ks, :] += lax.dot_general(act, ub, across, preferred_element_type=f32)
            gf = lax.dot_general(gp, mb, across, preferred_element_type=f32)
            gf_ref[ks, :] += gf
            second = second + jnp.sum((gf * w1f_ref[ks, :]).reshape(-1, 8, padded), axis=0)
            part = jnp.dot(w1t_ref[:, ks], gp, preferred_element_type=f32)
            total = part if total is None else total + part
        rounded = total.astype(jnp.bfloat16)
        gmix[b] = rounded
        dots = lax.dot_general(vec_ref[...], rounded, across, preferred_element_type=f32)
        second = jnp.sum(second, axis=0, keepdims=True)
        sums_ref[0, pl.ds(b, 1), :padded] = dots[0:1] + dots[1:2]
        sums_ref[1, pl.ds(b, 1), :padded] = second - (dots[2:3] + dots[3:4])
        return 0

    lax.fori_loop(0, images, image, 0, unroll=2)

    def post(i, _):
        first = pl.multiple_of(i * T, T)
        gm_ref[pl.ds(first, T)] = jnp.swapaxes(gmix[:, pl.ds(first, T), :], 0, 1)
        return 0

    lax.fori_loop(0, full, post, 0)
    if tail:
        tile = jnp.swapaxes(gmix[:, start:padded, :], 0, 1)
        gm_ref[start:] = tile[:tail]


def final_kernel(x_ref, up_ref, gm_ref, stat_ref, sums_ref, gain_ref, out_ref, chan_ref):
    i = pl.program_id(0)
    rows = x_ref.shape[0]
    width = stat_ref.shape[2]
    gain = gain_ref[...]

    @pl.when(i == 0)
    def _():
        chan_ref[...] = jnp.zeros_like(chan_ref)

    shift = lax.rem(width - i * rows, width)
    mean, inv = pltpu.roll(stat_ref[0], shift, 1), pltpu.roll(stat_ref[1], shift, 1)
    s1, s2 = pltpu.roll(sums_ref[0], shift, 1), pltpu.roll(sums_ref[1], shift, 1)
    products = jnp.zeros(x_ref.shape[1:], jnp.float32)
    plain = jnp.zeros(x_ref.shape[1:], jnp.float32)
    for j in range(rows):
        c = slice(j, j + 1)
        x = x_ref[j].astype(jnp.float32)
        normed = (x - mean[:, c]) * inv[:, c]
        t = gm_ref[j].astype(jnp.float32)
        products = products + t * normed
        plain = plain + t
        inner = t * gain - s1[:, c] - normed * s2[:, c]
        out_ref[j] = (up_ref[j].astype(jnp.float32) + inv[:, c] * inner).astype(jnp.bfloat16)
    chan_ref[0:1, :] += jnp.sum(products, axis=0, keepdims=True)
    chan_ref[1:2, :] += jnp.sum(plain, axis=0, keepdims=True)


def reduce_kernel(scale, first_ref, second_ref, chan_ref, *rest):
    first_out, second_out, bias_out, chan_out_ref, *scratch = rest
    patches = first_out.shape[1]
    one, one_c, held, held_c, two, two_c, own, three, sems, sems2, sems3 = scratch
    me, col = lax.axis_index("dp"), lax.axis_index("chan")
    n_dp, n_chan = lax.axis_size("dp"), lax.axis_size("chan")
    halves = n_dp // 2
    mine, core = me // 2, me % 2
    partner = me + 1 - 2 * core
    peers = [((mine + j) % halves) * 2 + core for j in range(1, halves)]
    columns = [(col + s) % n_chan for s in range(1, n_chan)]
    mesh_id = pl.DeviceIdType.MESH

    barrier = pltpu.get_barrier_semaphore()
    for d in [partner] + peers:
        pl.semaphore_signal(barrier, inc=1, device_id=(d, col), device_id_type=mesh_id)
    for d in columns:
        pl.semaphore_signal(barrier, inc=1, device_id=(me, d), device_id_type=mesh_id)
    pl.semaphore_wait(barrier, halves + n_chan - 1)

    def send(src, dst, sem, k, target):
        copy = pltpu.make_async_remote_copy(
            src_ref=src,
            dst_ref=dst,
            send_sem=sem.at[0, k],
            recv_sem=sem.at[1, k],
            device_id=target,
            device_id_type=mesh_id,
        )
        copy.start()
        return copy

    copies = [
        send(first_ref.at[:, 1 - core], one.at[0], sems, 0, (partner, col)),
        send(second_ref.at[:, 1 - core], one.at[1], sems, 1, (partner, col)),
        send(chan_ref, one_c, sems, 2, (partner, col)),
    ]
    for c in copies:
        c.wait()

    def add(t, _):
        held[t, 0] = first_ref[t, core] + one[0, t]
        held[t, 1] = second_ref[t, core] + one[1, t]
        return 0

    lax.fori_loop(0, halves, add, 0)
    held_c[...] = chan_ref[...] + one_c[...]
    copies = []
    for j in range(1, halves):
        t = (mine + j) % halves
        copies.append(send(held.at[t], two.at[j - 1], sems2, 2 * j - 2, (2 * t + core, col)))
        copies.append(send(held_c, two_c.at[mine], sems2, 2 * j - 1, (2 * t + core, col)))
    two_c[mine] = held_c[...]
    for c in copies:
        c.wait()
    total = held[mine]
    for j in range(1, halves):
        total = total + two[j - 1]
    own[...] = total
    copies = [
        send(own, three.at[col], sems3, s, (me, d)) for s, d in enumerate(columns)
    ]
    three[col] = total
    chan_sum = two_c[0]
    for j in range(1, halves):
        chan_sum = chan_sum + two_c[j]
    chan_out_ref[...] = chan_sum * scale
    for c in copies:
        c.wait()
    total = three[0]
    for j in range(1, n_chan):
        total = total + three[j]
    first_out[...] = total[0, :, :patches] * scale
    second_out[...] = total[1, :, :patches] * (0.5 * scale)
    bias_out[...] = total[0, :, patches : patches + 1] * scale


def reduce_all(first, second, chan, patches, scale):
    n_dp, n_chan = lax.axis_size("dp"), lax.axis_size("chan")
    halves = n_dp // 2
    rows, lanes = first.shape[0] // n_dp, first.shape[1]
    f32 = jnp.float32
    S = jax.ShapeDtypeStruct
    vmem = pl.BlockSpec(memory_space=pltpu.VMEM)
    shape = (halves, 2, rows, lanes)
    dma = pltpu.SemaphoreType.DMA
    return pl.pallas_call(
        functools.partial(reduce_kernel, scale),
        in_specs=[vmem] * 3,
        out_specs=[vmem] * 4,
        out_shape=[
            S((rows, patches), f32),
            S((rows, patches), f32),
            S((rows, 1), f32),
            S(chan.shape, f32),
        ],
        scratch_shapes=[
            pltpu.VMEM((2, halves, rows, lanes), f32),
            pltpu.VMEM(chan.shape, f32),
            pltpu.VMEM(shape, f32),
            pltpu.VMEM(chan.shape, f32),
            pltpu.VMEM((halves - 1, 2, rows, lanes), f32),
            pltpu.VMEM((halves,) + chan.shape, f32),
            pltpu.VMEM((2, rows, lanes), f32),
            pltpu.VMEM((n_chan, 2, rows, lanes), f32),
            dma((2, 3)),
            dma((2, 2 * halves - 2)),
            dma((2, n_chan - 1)),
        ],
        compiler_params=pltpu.CompilerParams(collective_id=0, has_side_effects=True),
    )(first.reshape(shape), second.reshape(shape), chan)


def others(x, axis):
    n = lax.axis_size(axis)
    return [x] + [
        lax.ppermute(x, axis, [(i, (i + s) % n) for i in range(n)]) for s in range(1, n)
    ]


def per_device(inputs, norm_gain, norm_bias, w_first, b_first, w_second, upstream):
    f32 = jnp.float32
    batch, patches, chans = inputs.shape
    hidden = w_first.shape[0]
    n_chan, n_dp = lax.axis_size("chan"), lax.axis_size("dp")
    width = chans * n_chan
    scale = 1.0 / (batch * n_dp)
    padded = -(-(patches + 3) // T) * T
    x = jnp.transpose(inputs, (1, 0, 2))
    up = jnp.transpose(upstream, (1, 0, 2))
    rows = max(r for r in range(1, T + 1) if patches % r == 0)
    steps = patches // rows
    S = jax.ShapeDtypeStruct
    params = functools.partial(pltpu.CompilerParams, dimension_semantics=("arbitrary",))

    local = pl.pallas_call(
        stats_kernel,
        grid=(steps,),
        in_specs=[pl.BlockSpec((rows, batch, chans), lambda i: (i, 0, 0))],
        out_specs=pl.BlockSpec((2, batch, LANES), lambda i: (0, 0, 0)),
        out_shape=S((2, batch, LANES), f32),
        compiler_params=params(),
    )(x)
    every = others(local, "chan")
    mean = sum(e[0] for e in every) / n_chan
    squares = sum(e[1] for e in every) + chans * sum(
        (e[0] - mean) * (e[0] - mean) for e in every
    )
    stat = jnp.stack([mean, lax.rsqrt(squares / width + epsilon)])

    high = lax.reduce_precision(b_first, 8, 7)
    middle = lax.reduce_precision(b_first - high, 8, 7)
    low = b_first - high - middle
    extra = jnp.stack([high, middle, low], axis=1).astype(jnp.bfloat16)
    w1 = jnp.concatenate([w_first, extra], axis=1)
    w1 = jnp.pad(w1, ((0, 0), (0, padded - patches - 3)))
    w1t = jnp.pad(w_first.T, ((0, padded - patches), (0, 0)))
    w2t = jnp.pad(0.5 * w_second.T, ((0, 0), (0, padded - patches)))
    w1f = w1t.T.astype(f32)
    gain2, bias2 = norm_gain[None, :], norm_bias[None, :]
    lead = lax.reduce_precision(jnp.stack([norm_gain, norm_bias]), 8, 7)
    rest = jnp.stack([norm_gain, norm_bias]) - lead
    vec = jnp.stack([lead[0], rest[0], lead[1], rest[1]]).astype(jnp.bfloat16)
    vec = jnp.pad(vec, ((0, T - 4), (0, 0)))

    whole = lambda shape: pl.BlockSpec(shape, lambda g: (0,) * len(shape))
    group = T
    big = pl.BlockSpec((patches, group, chans), lambda g: (0, g, 0))
    pair = pl.BlockSpec((2, group, LANES), lambda g: (0, g, 0))
    gm, sums, gf, gs = pl.pallas_call(
        functools.partial(main_kernel, patches),
        grid=(batch // group,),
        in_specs=[
            big,
            big,
            pair,
            whole((1, chans)),
            whole((1, chans)),
            whole((hidden, padded)),
            whole((padded, hidden)),
            whole((hidden, padded)),
            whole((hidden, padded)),
            whole((T, chans)),
        ],
        out_specs=[big, pair, whole((hidden, padded)), whole((hidden, padded))],
        out_shape=[
            S((patches, batch, chans), jnp.bfloat16),
            S((2, batch, LANES), f32),
            S((hidden, padded), f32),
            S((hidden, padded), f32),
        ],
        scratch_shapes=[
            pltpu.VMEM((group, padded, chans), jnp.bfloat16),
            pltpu.VMEM((group, padded, chans), jnp.bfloat16),
            pltpu.VMEM((group, padded, chans), jnp.bfloat16),
        ],
        compiler_params=params(vmem_limit_bytes=56 * MIB),
    )(x, up, stat, gain2, bias2, w1, w1t, w2t, w1f, vec)

    sums = sum(others(sums, "chan")) / width

    pblock = pl.BlockSpec((rows, batch, chans), lambda i: (i, 0, 0))
    out, chan = pl.pallas_call(
        final_kernel,
        grid=(steps,),
        in_specs=[
            pblock,
            pblock,
            pblock,
            whole((2, batch, LANES)),
            whole((2, batch, LANES)),
            whole((1, chans)),
        ],
        out_specs=[pblock, whole((2, chans))],
        out_shape=[S((patches, batch, chans), jnp.bfloat16), S((2, chans), f32)],
        compiler_params=params(),
        cost_estimate=pl.CostEstimate(
            flops=12 * x.size, bytes_accessed=8 * x.size, transcendentals=0
        ),
    )(x, up, gm, stat, sums, gain2)

    first, second, bias, chan = reduce_all(gf, gs, chan, patches, scale)
    return (jnp.transpose(out, (1, 0, 2)), first, second.T, bias[:, 0], chan[0], chan[1])


def solution(mesh):
    in_specs = (P("dp", None, "chan"), P("chan"), P("chan"), P(), P(), P(), P("dp", None, "chan"))
    out_specs = (P("dp", None, "chan"), P("dp", None), P(None, "dp"), P("dp"), P("chan"), P("chan"))
    return jax.shard_map(
        per_device, mesh=mesh, in_specs=in_specs, out_specs=out_specs, check_vma=False
    )
```
